32 devices in a mesh: dp: 8 (over z, y), mp: 4 (over x, core).
Axes of the slice: x: 2, y: 2, z: 4, core: 2. Of those that a mesh axis runs over, the one named last changes fastest.
Arguments:
- noise_blocks: bfloat16 [64, 12800], P('dp'), may hold values from -6 to 6
- data_blocks: bfloat16 [64, 12800], P('dp'), may hold values from -6 to 6
- destination: int32 [64], replicated, may hold values from 0 to 63, as said below
- utt_blocks: int32 [8, 4], P('dp'), may hold values from 1 to 4, 8 in all within a row
- span_start: int32 [8, 4], P('dp'), may hold values from 0 to 19
- span_size: int32 [8, 4], P('dp'), may hold values from 44 to 64
- timestep: int32 [8, 4], P('dp'), may hold values from 1 to 63
- in_weight: bfloat16 [200, 1024], replicated, may hold values from -0.4375 to 0.4375
- norm_gain: bfloat16 [1024], replicated, may hold values from 0.5 to 1.5
- qkv_weight: bfloat16 [1024, 3, 512], P(None, None, 'mp'), may hold values from -4 to 4
- out_proj: bfloat16 [512, 1024], P('mp'), may hold values from -0.25 to 0.25
- final_gain: bfloat16 [1024], replicated, may hold values from 0.25 to 1.75
- vel_weight: bfloat16 [1024, 100], replicated, may hold values from -0.1875 to 0.1875
Outputs:
- grad_qkv: float32 [1024, 3, 512], P('dp', None, 'mp')
- grad_out: float32 [512, 1024], P('mp', 'dp')
The draws below stay inside these ranges and needn't reach their ends.
Inputs may be any that keep to these rules, and one draw needn't show every extreme that they name: `destination`: A permutation of the 64 bin positions; a device sends to each bin either none or exactly 1 of its blocks.
All inputs are finite; a program needn't handle non-finite values.
Results may differ from the reference program's by a relative error of at most 0.004.
Values may be sent and summed in bfloat16 or wider, within the bound.
A program may use at most 64 MiB of HBM per device.

```python
import math
import jax
import jax.numpy as jnp
import numpy as np
from jax import lax

D = 1024
MEL = 100
HEAD_DIM = 64
BLOCK = 128
BLK_DEV = 8
INNER_WIDTH = 512
TOTAL_BLK = 64
CAP = 1
UTT_BIN = 4
MAXLEN = 4
N_DP = 8
N_MP = 4


def draw_destination(key, part):
    first, second, third, fourth, fifth = jax.random.split(key, 5)
    groups = BLK_DEV // CAP
    shifts = jax.random.permutation(first, N_DP)[:groups].astype(jnp.int32)
    outer = jax.random.permutation(second, N_DP).astype(jnp.int32)
    inner = jax.random.permutation(third, N_DP).astype(jnp.int32)
    source_order = jax.vmap(lambda k: jax.random.permutation(k, BLK_DEV))(jax.random.split(fourth, N_DP)).astype(jnp.int32)
    slot_order = jax.vmap(lambda k: jax.random.permutation(k, BLK_DEV))(jax.random.split(fifth, N_DP)).astype(jnp.int32)
    group = source_order // CAP
    within = source_order % CAP
    source = jnp.arange(N_DP, dtype=jnp.int32)[:, None]
    target_bin = outer[(inner[source] + shifts[group]) % N_DP]
    slot = slot_order[target_bin, group * CAP + within]
    return (target_bin * BLK_DEV + slot).reshape(-1).astype(jnp.int32)


def draw_qkv_weight(key, part):
    first = jax.random.fold_in(jax.random.fold_in(key, 11), 0)
    base = jax.random.normal(first, (D, 3, INNER_WIDTH), jnp.float32) * D ** (-0.5)
    return jnp.clip(base, -4.0, 4.0).astype(jnp.bfloat16)


def touch_ends(result, stream_key, low, largest):
    extent = result.shape
    index_at = [jax.random.randint(jax.random.fold_in(stream_key, axis), (), 0, extent[axis]) for axis in range(len(extent))]
    result = result.at[tuple(index_at)].set(low)
    longest = extent.index(max(extent))
    index_at[longest] = (index_at[longest] + 1) % extent[longest]
    return result.at[tuple(index_at)].set(largest)


def block_scale(stream_key, dims, cuts, low, high):
    level, own = 1.0, jax.random.fold_in(stream_key, 6)
    for position, shards_of in cuts:
        draws = jnp.exp(jax.random.uniform(jax.random.fold_in(own, position), (shards_of,), jnp.float32, low / len(cuts), high / len(cuts)))
        level = level * jnp.repeat(draws, dims[position] // shards_of).reshape([-1 if axis == position else 1 for axis in range(len(dims))])
    return level


def profile(amount, total, limit, skew):
    loads = [(1 << 20) // math.isqrt(grade ** skew) + 1 for grade in range(2, amount + 1)]
    spare, counts = total - limit - (amount - 1), [1] * (amount - 1)
    while spare > 0:
        movable = [i for i in range(amount - 1) if counts[i] < limit]
        pool, budget = sum([loads[i] for i in movable]), spare
        for i in movable:
            more = min(limit - counts[i], max(1, budget * loads[i] // pool), spare)
            counts[i] = counts[i] + more
            spare = spare - more
    return np.array([limit] + counts)


def ragged_sizes(own_key, number_of, total, most, slope):
    if number_of == 2:
        one = jax.random.randint(own_key, (), max(1, total - most), min(most, total - 1) + 1)
        return jnp.stack([one, total - one])
    tallies = jnp.asarray(profile(number_of, total, most, slope), jnp.int32)
    couples = (number_of - 1) // 2
    giver, sink = tallies[1:1 + 2 * couples:2], tallies[2:2 + 2 * couples:2]
    slack = jnp.minimum(giver - 1, most - sink)
    moved = jax.random.randint(jax.random.fold_in(own_key, 1), (couples,), 0, 1 << 20) % (slack + 1)
    tallies = tallies.at[1:1 + 2 * couples:2].set(giver - moved).at[2:2 + 2 * couples:2].set(sink + moved)
    return tallies[jax.random.permutation(jax.random.fold_in(own_key, 2), number_of)]


def centred(stream_key, dims, scale, limit, pieces=(), kind=jnp.bfloat16):
    entries = jax.random.normal(stream_key, dims, jnp.float32) * scale
    if len(pieces) > 0:
        entries = block_scale(stream_key, dims, pieces, -0.22, 0.18) * entries
    return jnp.clip(entries, min=-limit, max=limit).astype(kind)


def setup_inputs(seed: int = 0) -> dict:
    arg_keys = jax.random.split(jax.random.key(seed), 14)
    noise_blocks = centred(arg_keys[0], (TOTAL_BLK, BLOCK * MEL), 1.0, 6.0, ((0, 8),))
    data_blocks = centred(arg_keys[1], (TOTAL_BLK, BLOCK * MEL), 1.0, 6.0, ((0, 8),))
    destination = draw_destination(jax.random.fold_in(arg_keys[13], 71), 0)
    utt_blocks = jax.vmap(lambda own: ragged_sizes(own, UTT_BIN, BLK_DEV, MAXLEN, 2))(jax.random.split(arg_keys[3], N_DP)).reshape((N_DP, UTT_BIN)).astype(jnp.int32)
    span_start = touch_ends(jax.random.randint(arg_keys[4], (N_DP, UTT_BIN), 0, 20), jax.random.fold_in(arg_keys[4], 1), 0, 19).astype(jnp.int32)
    span_size = touch_ends(jax.random.randint(arg_keys[5], (N_DP, UTT_BIN), 44, 65), jax.random.fold_in(arg_keys[5], 1), 44, 64).astype(jnp.int32)
    timestep = touch_ends(jax.random.randint(arg_keys[6], (N_DP, UTT_BIN), 1, 64), jax.random.fold_in(arg_keys[6], 1), 1, 63).astype(jnp.int32)
    in_weight = centred(arg_keys[7], (2 * MEL, D), (2 * MEL) ** -0.5, 0.4375)
    norm_gain = jnp.clip(1.0 + 0.1 * jax.random.normal(arg_keys[8], (D,), jnp.float32), 0.5, 1.5).astype(jnp.bfloat16)
    qkv_weight = draw_qkv_weight(jax.random.fold_in(arg_keys[13], 71), 0)
    out_proj = centred(arg_keys[10], (INNER_WIDTH, D), INNER_WIDTH ** -0.5, 0.25, ((0, 4),))
    final_gain = jnp.clip(1.0 + 0.15 * jax.random.normal(arg_keys[11], (D,), jnp.float32), 0.25, 1.75).astype(jnp.bfloat16)
    vel_weight = centred(arg_keys[12], (D, MEL), D ** -0.5, 0.1875)
    return dict(noise_blocks=noise_blocks, data_blocks=data_blocks, destination=destination, utt_blocks=utt_blocks, span_start=span_start, span_size=span_size, timestep=timestep, in_weight=in_weight, norm_gain=norm_gain, qkv_weight=qkv_weight, out_proj=out_proj, final_gain=final_gain, vel_weight=vel_weight)


def frame_table(lengths, starts, sizes, steps, rows):
    lengths = lengths.astype(jnp.int32)
    ends = jnp.cumsum(lengths).astype(jnp.int32)
    frame = jnp.arange(rows, dtype=jnp.int32)
    block_index = frame // BLOCK
    segment = lax.optimization_barrier(jnp.sum((block_index[:, None] >= ends[None, :]).astype(jnp.int32), axis=1))
    member = segment[:, None] == jnp.arange(lengths.shape[0], dtype=jnp.int32)[None, :]
    first = lax.optimization_barrier(jnp.sum(jnp.where(member, (ends - lengths)[None, :], 0), axis=1)) * BLOCK
    span = lax.optimization_barrier(jnp.sum(jnp.where(member, lengths[None, :], 0), axis=1)) * BLOCK
    lower = lax.optimization_barrier(jnp.sum(jnp.where(member, starts[None, :], 0), axis=1))
    upper = lower + lax.optimization_barrier(jnp.sum(jnp.where(member, sizes[None, :], 0), axis=1))
    inside = 64 * (frame - first)
    masked = ((inside >= lower * span) & (inside < upper * span)).astype(jnp.float32)
    level = lax.optimization_barrier(jnp.sum(jnp.where(member, steps[None, :], 0), axis=1)).astype(jnp.float32) / 64.0
    return (segment, masked, level)

def attend(query, keys, values, segment):
    rows, width = query.shape
    heads = width // HEAD_DIM
    block = min(512, rows)
    reach = min(4, rows // BLOCK // 2) * BLOCK
    window = min(rows, block + 2 * reach)
    blocks = rows // block
    query_blocks = query.reshape(blocks, block, heads, HEAD_DIM)
    segment_blocks = segment.reshape(blocks, block)
    firsts = jnp.clip(jnp.arange(blocks, dtype=jnp.int32) * block - reach, 0, rows - window).astype(jnp.int32)
    keyed = keys.reshape(rows, heads, HEAD_DIM)
    valued = values.reshape(rows, heads, HEAD_DIM)

    def one_block(item):
        query_block, segment_block, first = item
        key_block = lax.dynamic_slice_in_dim(keyed, first, window, 0)
        value_block = lax.dynamic_slice_in_dim(valued, first, window, 0)
        key_segment = lax.dynamic_slice_in_dim(segment, first, window, 0)
        scores = jnp.einsum('qhd,khd->hqk', query_block, key_block, preferred_element_type=jnp.float32) * HEAD_DIM ** (-0.5)
        scores = jnp.where((segment_block[:, None] == key_segment[None, :])[None], scores, -1e+30)
        top = lax.optimization_barrier(jnp.max(scores, axis=-1, keepdims=True))
        weights = jnp.exp(scores - top)
        probs = (weights / lax.optimization_barrier(jnp.sum(weights, axis=-1, keepdims=True))).astype(jnp.bfloat16)
        return jnp.einsum('hqk,khd->qhd', probs, value_block, preferred_element_type=jnp.float32).reshape(block, width)
    return lax.map(jax.checkpoint(one_block), (query_blocks, segment_blocks, firsts)).reshape(rows, width)

def reference(noise_blocks, data_blocks, destination, utt_blocks, span_start, span_size, timestep, in_weight, norm_gain, qkv_weight, out_proj, final_gain, vel_weight):
    total = noise_blocks.shape[0]
    bins = utt_blocks.shape[0]
    per_bin = total // bins
    rows = per_bin * BLOCK
    mel = noise_blocks.shape[1] // BLOCK
    ordered_noise = jnp.zeros_like(noise_blocks).at[destination].set(noise_blocks)
    ordered_data = jnp.zeros_like(data_blocks).at[destination].set(data_blocks)
    group_width = INNER_WIDTH // N_MP
    gain_out = final_gain.astype(jnp.float32)[None, :]

    def one_bin(carry, index):
        grad_qkv, grad_out, count = carry
        noise = lax.dynamic_slice_in_dim(ordered_noise, index * per_bin, per_bin, 0).reshape(rows, mel).astype(jnp.float32)
        data = lax.dynamic_slice_in_dim(ordered_data, index * per_bin, per_bin, 0).reshape(rows, mel).astype(jnp.float32)
        lengths = lax.dynamic_index_in_dim(utt_blocks, index, 0, keepdims=False)
        starts = lax.dynamic_index_in_dim(span_start, index, 0, keepdims=False)
        sizes = lax.dynamic_index_in_dim(span_size, index, 0, keepdims=False)
        steps = lax.dynamic_index_in_dim(timestep, index, 0, keepdims=False)
        segment, masked, level = frame_table(lengths, starts, sizes, steps, rows)
        noisy = (1.0 - level[:, None]) * noise + level[:, None] * data
        cond = data * (1.0 - masked[:, None])
        target = data - noise
        inputs = jnp.concatenate([noisy, cond], axis=1).astype(jnp.bfloat16)
        hidden0 = jnp.dot(inputs, in_weight, preferred_element_type=jnp.float32)
        scale = lax.rsqrt(lax.optimization_barrier(jnp.mean(hidden0 * hidden0, axis=1, keepdims=True)) + 1e-06)
        normed = (hidden0 * scale * norm_gain.astype(jnp.float32)[None, :]).astype(jnp.bfloat16)
        query = jnp.dot(normed, qkv_weight[:, 0, :], preferred_element_type=jnp.float32).astype(jnp.bfloat16)
        keys = jnp.dot(normed, qkv_weight[:, 1, :], preferred_element_type=jnp.float32).astype(jnp.bfloat16)
        values = jnp.dot(normed, qkv_weight[:, 2, :], preferred_element_type=jnp.float32).astype(jnp.bfloat16)
        heads_out, pullback = jax.vjp(lambda a, b, c: attend(a, b, c, segment), query, keys, values)
        attended = heads_out.astype(jnp.bfloat16)
        mixed = jnp.zeros((rows, D), jnp.float32)
        for group in range(N_MP):
            lo = group * group_width
            part = jnp.dot(attended[:, lo:lo + group_width], out_proj[lo:lo + group_width, :], preferred_element_type=jnp.float32)
            mixed = mixed + part.astype(jnp.bfloat16).astype(jnp.float32)
        hidden1 = (hidden0 + mixed).astype(jnp.bfloat16)
        wide1 = lax.optimization_barrier(hidden1).astype(jnp.float32)
        rscale = lax.rsqrt(lax.optimization_barrier(jnp.mean(wide1 * wide1, axis=1, keepdims=True)) + 1e-06)
        normalized = wide1 * rscale
        final = (normalized * gain_out).astype(jnp.bfloat16)
        velocity = jnp.dot(final, vel_weight, preferred_element_type=jnp.float32)
        error = (2.0 * masked[:, None] * (velocity - target)).astype(jnp.bfloat16)
        grad_final = jnp.dot(error, vel_weight.T, preferred_element_type=jnp.float32)
        scaled = grad_final * gain_out
        back1 = (rscale * (scaled - normalized * lax.optimization_barrier(jnp.mean(scaled * normalized, axis=1, keepdims=True)))).astype(jnp.bfloat16)
        back_att = jnp.dot(back1, out_proj.T, preferred_element_type=jnp.float32).astype(jnp.bfloat16)
        dquery, dkeys, dvalues = pullback(back_att.astype(jnp.float32))
        grad_out = grad_out + jnp.dot(attended.T, back1, preferred_element_type=jnp.float32)
        terms = jnp.stack([jnp.dot(normed.T, dquery, preferred_element_type=jnp.float32), jnp.dot(normed.T, dkeys, preferred_element_type=jnp.float32), jnp.dot(normed.T, dvalues, preferred_element_type=jnp.float32)], axis=1)
        return ((grad_qkv + terms, grad_out, count + jnp.sum(masked)), None)
    start = (jnp.zeros((D, 3, INNER_WIDTH), jnp.float32), jnp.zeros((INNER_WIDTH, D), jnp.float32), jnp.zeros((), jnp.float32))
    (grad_qkv, grad_out, count), _ = lax.scan(one_bin, start, jnp.arange(bins, dtype=jnp.int32))
    return (grad_qkv / count, grad_out / count)
```

```python
import functools

import jax
import jax.numpy as jnp
from jax import lax
from jax.experimental import pallas as pl
from jax.experimental.pallas import tpu as pltpu
from jax.sharding import PartitionSpec as P

HEAD_DIM = 64
BLOCK = 128
MESH = pl.DeviceIdType.MESH
VMEM = pl.BlockSpec(memory_space=pltpu.VMEM)
SMEM = pl.BlockSpec(memory_space=pltpu.SMEM)
F32, BF16 = jnp.float32, jnp.bfloat16
NT = (((1,), (1,)), ((), ()))
TN = (((0,), (0,)), ((), ()))


def dot(a, b, dims=(((1,), (0,)), ((), ()))):
    return lax.dot_general(a, b, dims, preferred_element_type=F32)


def params(**kw):
    return pltpu.CompilerParams(vmem_limit_bytes=56 * 2**20, **kw)


def greet(dp, mp, with_dp, with_mp):
    me, my = lax.axis_index("dp"), lax.axis_index("mp")
    barrier = pltpu.get_barrier_semaphore()
    n = 0
    if with_dp:
        for i in range(1, dp):
            pl.semaphore_signal(
                barrier, inc=1, device_id=(lax.rem(me + i, dp), my), device_id_type=MESH
            )
        n += dp - 1
    if with_mp:
        for i in range(1, mp):
            pl.semaphore_signal(
                barrier, inc=1, device_id=(me, lax.rem(my + i, mp)), device_id_type=MESH
            )
        n += mp - 1
    return lambda: pl.semaphore_wait(barrier, n)


def gather_mp(mp, src, dst_at, local, send, recv, fsend, frecv):
    me, my = lax.axis_index("dp"), lax.axis_index("mp")
    pair, side = my // 2, lax.rem(my, 2)
    mate = pair * 2 + 1 - side
    keep = pltpu.make_async_copy(src, dst_at(my), local)
    direct = []
    for c in range(1, mp // 2):
        far = lax.rem(pair + c, mp // 2) * 2 + side
        direct.append(
            pltpu.make_async_remote_copy(
                src, dst_at(my), send.at[c], recv.at[c], device_id=(me, far), device_id_type=MESH
            )
        )
    near = pltpu.make_async_remote_copy(
        src, dst_at(my), send.at[0], recv.at[0], device_id=(me, mate), device_id_type=MESH
    )

    def start():
        for d in direct:
            d.start()
        near.start()
        keep.start()

    def finish():
        onward = []
        for c, d in enumerate(direct, 1):
            d.wait_recv()
            origin = lax.rem(pair + mp // 2 - c, mp // 2) * 2 + side
            f = pltpu.make_async_remote_copy(
                dst_at(origin), dst_at(origin), fsend.at[c], frecv.at[c],
                device_id=(me, mate), device_id_type=MESH,
            )
            f.start()
            onward.append(f)
        near.wait()
        keep.wait()
        for d in direct:
            d.wait_send()
        for f in onward:
            f.wait()

    return start, finish


def load_kernel(
    dp, mp, pick_ref, from_ref, utt_ref, start_ref, size_ref, x_ref, w_ref,
    bin_ref, full_ref, count_ref,
    stage, got, tally, send, recv, csend, crecv, local, ssend, srecv, fsend, frecv,
):
    me, my = lax.axis_index("dp"), lax.axis_index("mp")
    wait = greet(dp, mp, True, True)
    for i in range(dp):
        stage[i] = x_ref[pick_ref[lax.rem(me + i, dp)]]
    count = jnp.int32(0)
    for u in range(utt_ref.shape[1]):
        low = start_ref[0, u]
        high = jnp.minimum(low + size_ref[0, u], 64)
        count += (high - low) * utt_ref[0, u] * (BLOCK // 64)
    tally[me] = jnp.full(tally.shape[1:], count, jnp.int32).astype(F32)
    wait()
    rows = w_ref.shape[0]
    start, finish = gather_mp(
        mp, w_ref, lambda i: full_ref.at[pl.ds(pl.multiple_of(i * rows, rows), rows)],
        local, ssend, srecv, fsend, frecv,
    )
    copies = []
    for i in range(1, dp):
        to = lax.rem(me + i, dp)
        copies.append(
            pltpu.make_async_remote_copy(
                stage.at[i], got.at[me], send.at[i], recv.at[i],
                device_id=(to, my), device_id_type=MESH,
            )
        )
        copies.append(
            pltpu.make_async_remote_copy(
                tally.at[me], tally.at[me], csend.at[i], crecv.at[i],
                device_id=(to, my), device_id_type=MESH,
            )
        )
    for c in copies:
        c.start()
    start()
    got[me] = stage[0]
    finish()
    for c in copies:
        c.wait()
    for j in range(bin_ref.shape[0]):
        bin_ref[j] = got[from_ref[j]]
    count_ref[...] = jnp.sum(tally[...], axis=0)


def gather_kernel(dp, mp, a_ref, out_ref, local, send, recv, fsend, frecv):
    greet(dp, mp, False, True)()
    start, finish = gather_mp(mp, a_ref, lambda i: out_ref.at[i], local, send, recv, fsend, frecv)
    start()
    finish()


def reduce_kernel(dp, mp, qkv_ref, o_ref, qkv_out, o_out, gq, go, sq, rq, so, ro):
    me, my = lax.axis_index("dp"), lax.axis_index("mp")
    greet(dp, mp, True, False)()
    rows = qkv_out.shape[0]

    def part(ref, i):
        return ref.at[pl.ds(pl.multiple_of(i * rows, rows), rows)]

    copies = []
    for i in range(1, dp):
        to = lax.rem(me + i, dp)
        for ref, got, s, r in ((qkv_ref, gq, sq, rq), (o_ref, go, so, ro)):
            copies.append(
                pltpu.make_async_remote_copy(
                    part(ref, to), got.at[i - 1], s.at[i], r.at[i],
                    device_id=(to, my), device_id_type=MESH,
                )
            )
    for c in copies:
        c.start()
    qkv_out[...] = part(qkv_ref, me)[...].astype(F32)
    o_out[...] = part(o_ref, me)[...].astype(F32)
    for i in range(1, dp):
        copies[2 * i - 2].wait()
        copies[2 * i - 1].wait()
        qkv_out[...] += gq[i - 1].astype(F32)
        o_out[...] += go[i - 1].astype(F32)


def segment_of(utt_ref, b):
    first, length, at = jnp.int32(0), jnp.int32(0), jnp.int32(0)
    for u in range(utt_ref.shape[1]):
        n = utt_ref[0, u]
        inside = (b >= at) & (b < at + n)
        first = jnp.where(inside, at, first)
        length = jnp.where(inside, n, length)
        at = at + n
    return first, length


def head_masks(width):
    lane = lax.broadcasted_iota(jnp.int32, (1, width), 1) // HEAD_DIM
    return [lane == h for h in range(width // HEAD_DIM)]


def for_blocks(utt_ref, blocks, longest, body):
    def step(b, _):
        first, length = segment_of(utt_ref, b)
        rows = pl.ds(pl.multiple_of(b * BLOCK, BLOCK), BLOCK)
        for n in range(1, longest + 1):
            @pl.when(length == n)
            def _():
                body(rows, pl.ds(pl.multiple_of(first * BLOCK, BLOCK), n * BLOCK))
        return 0

    lax.fori_loop(0, blocks, step, 0)


def softmax(s):
    e = jnp.exp(s - jnp.max(s, axis=1, keepdims=True))
    return e / jnp.sum(e, axis=1, keepdims=True)


def attend_kernel(longest, utt_ref, q_ref, k_ref, v_ref, out_ref):
    masks = head_masks(q_ref.shape[1])

    def body(rows, keys):
        q, k, v = q_ref[rows] * BF16(HEAD_DIM**-0.5), k_ref[keys], v_ref[keys]
        out = None
        for m in masks:
            p = softmax(dot(jnp.where(m, q, BF16(0)), k, NT)).astype(BF16)
            o = dot(p, v)
            out = o if out is None else jnp.where(m, o, out)
        out_ref[rows] = out.astype(BF16)

    for_blocks(utt_ref, q_ref.shape[0] // BLOCK, longest, body)


def pullback_kernel(longest, utt_ref, q_ref, k_ref, v_ref, do_ref, d_ref, dk, dv):
    width = q_ref.shape[1]
    masks = head_masks(width)
    dk[...] = jnp.zeros_like(dk)
    dv[...] = jnp.zeros_like(dv)
    scale = HEAD_DIM**-0.5

    def body(rows, keys):
        q, k, v = q_ref[rows] * BF16(scale), k_ref[keys], v_ref[keys]
        do = do_ref[rows]
        dq = None
        for m in masks:
            qh = jnp.where(m, q, BF16(0))
            doh = jnp.where(m, do, BF16(0))
            p = softmax(dot(qh, k, NT))
            dp = dot(doh, v, NT).astype(BF16).astype(F32)
            ds = (p * (dp - jnp.sum(dp * p, axis=1, keepdims=True))).astype(BF16)
            g = dot(ds, k)
            dq = g if dq is None else jnp.where(m, g, dq)
            dk[keys] += dot(ds, qh, TN)
            dv[keys] += dot(p.astype(BF16), doh, TN)
        d_ref[rows, :width] = (dq * scale).astype(BF16)

    for_blocks(utt_ref, q_ref.shape[0] // BLOCK, longest, body)
    d_ref[:, width : 2 * width] = dk[...].astype(BF16)
    d_ref[:, 2 * width :] = dv[...].astype(BF16)


def shards(
    dp, mp, noise_blocks, data_blocks, destination, utt_blocks, span_start, span_size, timestep,
    in_weight, norm_gain, qkv_weight, out_proj, final_gain, vel_weight,
):
    me = lax.axis_index("dp")
    per_dev = noise_blocks.shape[0]
    rows = per_dev * BLOCK
    mel = noise_blocks.shape[1] // BLOCK
    features = in_weight.shape[1]
    width = qkv_weight.shape[2]
    longest = min(4, per_dev)
    order = jnp.arange(per_dev, dtype=jnp.int32)
    mine = lax.dynamic_slice_in_dim(destination, me * per_dev, per_dev) // per_dev
    pick = jnp.sum(
        jnp.where(mine[None, :] == jnp.arange(dp, dtype=jnp.int32)[:, None], order[None, :], 0), axis=1
    )
    source = jnp.arange(destination.shape[0], dtype=jnp.int32) // per_dev
    origin = jnp.sum(
        jnp.where(destination[None, :] == (me * per_dev + order)[:, None], source[None, :], 0), axis=1
    )
    frames = jnp.concatenate(
        [noise_blocks.reshape(per_dev, BLOCK, mel), data_blocks.reshape(per_dev, BLOCK, mel)], axis=2
    )
    dma = pltpu.SemaphoreType.DMA
    bins, out_full, count = pl.pallas_call(
        functools.partial(load_kernel, dp, mp),
        out_shape=(
            jax.ShapeDtypeStruct(frames.shape, BF16),
            jax.ShapeDtypeStruct((mp * width, features), BF16),
            jax.ShapeDtypeStruct((8, 128), F32),
        ),
        in_specs=[SMEM] * 5 + [VMEM] * 2,
        out_specs=(VMEM,) * 3,
        scratch_shapes=[
            pltpu.VMEM((dp,) + frames.shape[1:], BF16),
            pltpu.VMEM((dp,) + frames.shape[1:], BF16),
            pltpu.VMEM((dp, 8, 128), F32),
            dma((dp,)), dma((dp,)), dma((dp,)), dma((dp,)), dma(()),
            dma((mp,)), dma((mp,)), dma((mp,)), dma((mp,)),
        ],
        compiler_params=params(collective_id=0, has_side_effects=True),
        name="load_blocks",
    )(pick, origin, utt_blocks, span_start, span_size, frames, out_proj)

    lengths = utt_blocks[0]
    ends = jnp.cumsum(lengths)
    frame = jnp.arange(rows, dtype=jnp.int32)
    block = frame // BLOCK
    member = (block[:, None] >= (ends - lengths)[None, :]) & (block[:, None] < ends[None, :])
    first = (ends - lengths) * BLOCK
    inside = 64 * (frame[:, None] - first[None, :])
    span = lengths * BLOCK
    low, high = span_start[0] * span, (span_start[0] + span_size[0]) * span
    masked = jnp.sum(
        (member & (inside >= low[None, :]) & (inside < high[None, :])).astype(F32), axis=1
    )
    level = jnp.sum(jnp.where(member, timestep[0][None, :], 0), axis=1).astype(F32) / 64.0

    frames = bins.reshape(rows, 2 * mel).astype(F32)
    noise, data = frames[:, :mel], frames[:, mel:]
    noisy = (1.0 - level[:, None]) * noise + level[:, None] * data
    cond = data * (1.0 - masked[:, None])
    target = data - noise
    inputs = jnp.concatenate([noisy, cond], axis=1).astype(BF16)
    hidden0 = dot(inputs, in_weight)
    scale = lax.rsqrt(jnp.mean(hidden0 * hidden0, axis=1, keepdims=True) + 1e-06)
    normed = (hidden0 * scale * norm_gain.astype(F32)[None, :]).astype(BF16)
    query = dot(normed, qkv_weight[:, 0, :]).astype(BF16)
    keys = dot(normed, qkv_weight[:, 1, :]).astype(BF16)
    values = dot(normed, qkv_weight[:, 2, :]).astype(BF16)

    attended = pl.pallas_call(
        functools.partial(attend_kernel, longest),
        out_shape=jax.ShapeDtypeStruct((rows, width), BF16),
        in_specs=[SMEM] + [VMEM] * 3,
        out_specs=VMEM,
        compiler_params=params(),
        name="attend",
    )(utt_blocks, query, keys, values)
    everyone = pl.pallas_call(
        functools.partial(gather_kernel, dp, mp),
        out_shape=jax.ShapeDtypeStruct((mp, rows, width), BF16),
        in_specs=[VMEM],
        out_specs=VMEM,
        scratch_shapes=[dma(()), dma((mp,)), dma((mp,)), dma((mp,)), dma((mp,))],
        compiler_params=params(collective_id=1, has_side_effects=True),
        name="gather_attended",
    )(attended)
    mixed = None
    for g in range(mp):
        part = dot(everyone[g], out_full[g * width : (g + 1) * width]).astype(BF16).astype(F32)
        mixed = part if mixed is None else mixed + part
    hidden1 = (hidden0 + mixed).astype(BF16)
    wide1 = lax.optimization_barrier(hidden1).astype(F32)
    rscale = lax.rsqrt(jnp.mean(wide1 * wide1, axis=1, keepdims=True) + 1e-06)
    normalized = wide1 * rscale
    gain_out = final_gain.astype(F32)[None, :]
    final = (normalized * gain_out).astype(BF16)
    velocity = dot(final, vel_weight)
    error = (2.0 * masked[:, None] * (velocity - target)).astype(BF16)
    grad_final = dot(error, vel_weight.T)
    scaled = grad_final * gain_out
    back1 = (
        rscale * (scaled - normalized * jnp.mean(scaled * normalized, axis=1, keepdims=True))
    ).astype(BF16)
    back_att = dot(back1, out_proj.T).astype(BF16)
    grads = pl.pallas_call(
        functools.partial(pullback_kernel, longest),
        out_shape=jax.ShapeDtypeStruct((rows, 3 * width), BF16),
        in_specs=[SMEM] + [VMEM] * 4,
        out_specs=VMEM,
        scratch_shapes=[pltpu.VMEM((rows, width), F32)] * 2,
        compiler_params=params(),
        name="attend_pullback",
    )(utt_blocks, query, keys, values, back_att)
    out_terms = dot(back1, attended, TN).astype(BF16)
    qkv_terms = dot(normed, grads, TN).astype(BF16)
    share = features // dp
    summed_qkv, summed_out = pl.pallas_call(
        functools.partial(reduce_kernel, dp, mp),
        out_shape=(
            jax.ShapeDtypeStruct((share, 3 * width), F32),
            jax.ShapeDtypeStruct((share, width), F32),
        ),
        in_specs=[VMEM] * 2,
        out_specs=(VMEM,) * 2,
        scratch_shapes=[
            pltpu.VMEM((dp - 1, share, 3 * width), BF16),
            pltpu.VMEM((dp - 1, share, width), BF16),
            dma((dp,)), dma((dp,)), dma((dp,)), dma((dp,)),
        ],
        compiler_params=params(collective_id=2, has_side_effects=True),
        name="reduce_grads",
    )(qkv_terms, out_terms)
    total = count[0, 0]
    return (summed_qkv.reshape(share, 3, width) / total, summed_out.T / total)


def solution(mesh):
    in_specs = (
        P("dp", None), P("dp", None), P(), P("dp", None), P("dp", None), P("dp", None),
        P("dp", None), P(), P(), P(None, None, "mp"), P("mp", None), P(), P(),
    )
    out_specs = (P("dp", None, "mp"), P("mp", "dp"))
    return jax.shard_map(
        functools.partial(shards, mesh.shape["dp"], mesh.shape["mp"]),
        mesh=mesh, in_specs=in_specs, out_specs=out_specs, check_vma=False,
    )
```

```python
import functools

import jax
import jax.numpy as jnp
from jax import lax
from jax.experimental import pallas as pl
from jax.experimental.pallas import tpu as pltpu
from jax.sharding import PartitionSpec as P

HEAD_DIM = 64
BLOCK = 128
MESH = pl.DeviceIdType.MESH
VMEM = pl.BlockSpec(memory_space=pltpu.VMEM)
SMEM = pl.BlockSpec(memory_space=pltpu.SMEM)
F32, BF16 = jnp.float32, jnp.bfloat16
NT = (((1,), (1,)), ((), ()))
TN = (((0,), (0,)), ((), ()))


def dot(a, b, dims=(((1,), (0,)), ((), ()))):
    return lax.dot_general(a, b, dims, preferred_element_type=F32)


def params(**kw):
    return pltpu.CompilerParams(vmem_limit_bytes=56 * 2**20, **kw)


def greet(dp, mp, with_dp, with_mp):
    me, my = lax.axis_index("dp"), lax.axis_index("mp")
    barrier = pltpu.get_barrier_semaphore()
    n = 0
    if with_dp:
        for i in range(1, dp):
            pl.semaphore_signal(
                barrier, inc=1, device_id=(lax.rem(me + i, dp), my), device_id_type=MESH
            )
        n += dp - 1
    if with_mp:
        for i in range(1, mp):
            pl.semaphore_signal(
                barrier, inc=1, device_id=(me, lax.rem(my + i, mp)), device_id_type=MESH
            )
        n += mp - 1
    return lambda: pl.semaphore_wait(barrier, n)


def gather_mp(mp, src, dst_at, local, send, recv, fsend, frecv):
    me, my = lax.axis_index("dp"), lax.axis_index("mp")
    pair, side = my // 2, lax.rem(my, 2)
    mate = pair * 2 + 1 - side
    keep = pltpu.make_async_copy(src, dst_at(my), local)
    direct = []
    for c in range(1, mp // 2):
        far = lax.rem(pair + c, mp // 2) * 2 + side
        direct.append(
            pltpu.make_async_remote_copy(
                src, dst_at(my), send.at[c], recv.at[c], device_id=(me, far), device_id_type=MESH
            )
        )
    near = pltpu.make_async_remote_copy(
        src, dst_at(my), send.at[0], recv.at[0], device_id=(me, mate), device_id_type=MESH
    )

    def start():
        for d in direct:
            d.start()
        near.start()
        keep.start()

    def finish():
        onward = []
        for c, d in enumerate(direct, 1):
            d.wait_recv()
            origin = lax.rem(pair + mp // 2 - c, mp // 2) * 2 + side
            f = pltpu.make_async_remote_copy(
                dst_at(origin), dst_at(origin), fsend.at[c], frecv.at[c],
                device_id=(me, mate), device_id_type=MESH,
            )
            f.start()
            onward.append(f)
        near.wait()
        keep.wait()
        for d in direct:
            d.wait_send()
        for f in onward:
            f.wait()

    return start, finish


def load_kernel(
    dp, mp, dest_ref, utt_ref, start_ref, size_ref, x_ref, w_ref,
    bin_ref, full_ref, count_ref,
    stage, got, tally, send, recv, csend, crecv, hsend, hrecv, local, ssend, srecv, fsend, frecv,
):
    me, my = lax.axis_index("dp"), lax.axis_index("mp")
    wait = greet(dp, mp, True, True)
    per_dev = bin_ref.shape[1]
    owners = [dest_ref[me * per_dev + k] // per_dev for k in range(per_dev)]
    for i in range(dp):
        to = lax.rem(me + i, dp)
        pick = jnp.int32(0)
        for k in range(per_dev):
            pick = jnp.where(owners[k] == to, k, pick)
        for part in range(2):
            stage[i, part] = x_ref[part, pick]
    count = jnp.int32(0)
    for u in range(utt_ref.shape[1]):
        low = start_ref[0, u]
        high = jnp.minimum(low + size_ref[0, u], 64)
        count += (high - low) * utt_ref[0, u] * (BLOCK // 64)
    tally[me] = jnp.full(tally.shape[1:], count, jnp.int32).astype(F32)
    side = lax.rem(my, 2)
    mate = my + 1 - 2 * side
    half = BLOCK // 2
    lines = pl.ds(pl.multiple_of(side * half, half), half)
    got[me, :, lines] = stage[0, :, lines]
    wait()
    rows = w_ref.shape[0]
    start, finish = gather_mp(
        mp, w_ref, lambda i: full_ref.at[pl.ds(pl.multiple_of(i * rows, rows), rows)],
        local, ssend, srecv, fsend, frecv,
    )
    frames, counts = [], []
    for i in range(1, dp):
        to = lax.rem(me + i, dp)
        frames.append(
            pltpu.make_async_remote_copy(
                stage.at[i, :, lines], got.at[me, :, lines], send.at[i], recv.at[i],
                device_id=(to, my), device_id_type=MESH,
            )
        )
        counts.append(
            pltpu.make_async_remote_copy(
                tally.at[me], tally.at[me], csend.at[i], crecv.at[i],
                device_id=(to, my), device_id_type=MESH,
            )
        )
    for c in frames + counts:
        c.start()
    start()
    onward = []
    for i in range(dp):
        if i > 0:
            frames[i - 1].wait_recv()
        slot = lax.rem(me + dp - i, dp)
        f = pltpu.make_async_remote_copy(
            got.at[slot, :, lines], got.at[slot, :, lines], hsend.at[i], hrecv.at[i],
            device_id=(me, mate), device_id_type=MESH,
        )
        f.start()
        onward.append(f)

    def find(i, found):
        d = dest_ref[i]
        return tuple(jnp.where(d == me * per_dev + j, i // per_dev, o) for j, o in enumerate(found))

    origin = lax.fori_loop(0, dp * per_dev, find, (jnp.int32(0),) * per_dev)
    finish()
    for c in frames:
        c.wait_send()
    for c in counts + onward:
        c.wait()
    for j in range(per_dev):
        for part in range(2):
            bin_ref[part, j] = got[origin[j], part]
    count_ref[...] = jnp.sum(tally[...], axis=0)


def gather_kernel(dp, mp, a_ref, out_ref, local, send, recv, fsend, frecv):
    greet(dp, mp, False, True)()
    start, finish = gather_mp(mp, a_ref, lambda i: out_ref.at[i], local, send, recv, fsend, frecv)
    start()
    finish()


def reduce_kernel(
    dp, mp, normed_ref, d_ref, back_ref, att_ref, count_ref, qkv_out, o_out,
    terms, near, sums, far, s1, r1, s2, r2,
):
    me, my = lax.axis_index("dp"), lax.axis_index("mp")
    ready = greet(dp, mp, True, False)
    rows, chunks, groups = o_out.shape[0], terms.shape[0], dp // 2
    group, side = me // 2, lax.rem(me, 2)
    mate = me + 1 - 2 * side
    width = o_out.shape[1]

    def block(j, g, s):
        return terms.at[j, pl.ds(pl.multiple_of((g * 2 + s) * rows, rows), rows)]

    first, second = [], []
    for j in range(chunks):
        if j == 0:
            t = dot(back_ref[...], att_ref[...], TN)
        else:
            t = dot(normed_ref[...], d_ref[:, (j - 1) * width : j * width], TN)
        terms[j] = t.astype(BF16)
        if j == 0:
            ready()
        out = []
        for i in range(groups):
            g = lax.rem(group + i, groups)
            out.append(
                pltpu.make_async_remote_copy(
                    block(j, g, 1 - side), near.at[j, g], s1.at[j, i], r1.at[j, i],
                    device_id=(mate, my), device_id_type=MESH,
                )
            )
        for c in out[1:] + out[:1]:
            c.start()
        first.append(out)

    def middle(j):
        for i in range(1, groups):
            g = lax.rem(group + i, groups)
            first[j][i].wait_recv()
            sums[j, i] = (block(j, g, side)[...].astype(F32) + near[j, g].astype(F32)).astype(BF16)
            c = pltpu.make_async_remote_copy(
                sums.at[j, i], far.at[j, i], s2.at[j, i], r2.at[j, i],
                device_id=(g * 2 + side, my), device_id_type=MESH,
            )
            c.start()
            second.append(c)
        first[j][0].wait_recv()

    def last(j):
        total = block(j, group, side)[...].astype(F32) + near[j, group].astype(F32)
        for i in range(1, groups):
            second[j * (groups - 1) + i - 1].wait_recv()
            total += far[j, i].astype(F32)
        total = total / count_ref[0:1, :]
        if j == 0:
            o_out[...] = total
        else:
            qkv_out[:, (j - 1) * width : j * width] = total

    for j in range(chunks):
        middle(j)
    for j in range(chunks):
        last(j)
    for out in first:
        for c in out:
            c.wait_send()
    for c in second:
        c.wait_send()


def utterances(utt_ref, longest, body):
    def step(u, at):
        length = utt_ref[0, u]
        for n in range(1, longest + 1):
            @pl.when(length == n)
            def _():
                body(pl.ds(pl.multiple_of(at * BLOCK, BLOCK), n * BLOCK))
        return at + length

    lax.fori_loop(0, utt_ref.shape[1], step, jnp.int32(0))


def span_table(utt_ref, start_ref, size_ref, step_ref, b):
    at = jnp.int32(0)
    offset = low = high = step = jnp.int32(0)
    for u in range(utt_ref.shape[1]):
        n = utt_ref[0, u]
        inside = (b >= at) & (b < at + n)
        lo = start_ref[0, u] * n * (BLOCK // 64)
        hi = (start_ref[0, u] + size_ref[0, u]) * n * (BLOCK // 64)
        offset = jnp.where(inside, (b - at) * BLOCK, offset)
        low = jnp.where(inside, lo, low)
        high = jnp.where(inside, hi, high)
        if step_ref is not None:
            step = jnp.where(inside, step_ref[0, u], step)
        at = at + n
    frame = offset + lax.broadcasted_iota(jnp.int32, (BLOCK, 1), 0)
    masked = ((frame >= low) & (frame < high)).astype(F32)
    return masked, step


def head_masks(width):
    lane = lax.broadcasted_iota(jnp.int32, (1, width), 1) // HEAD_DIM
    return [lane == h for h in range(width // HEAD_DIM)]


def softmax(s):
    e = jnp.exp(s - jnp.max(s, axis=1, keepdims=True))
    return e / jnp.sum(e, axis=1, keepdims=True)


def forward_kernel(
    longest, utt_ref, start_ref, size_ref, step_ref, bin_ref, win_ref, gain_ref, wqkv_ref,
    hidden_ref, normed_ref, qkv_ref, att_ref,
):
    width = att_ref.shape[1]
    gain = gain_ref[...].astype(F32)

    def block(b, _):
        rows = pl.ds(pl.multiple_of(b * BLOCK, BLOCK), BLOCK)
        masked, step = span_table(utt_ref, start_ref, size_ref, step_ref, b)
        noise, data = bin_ref[0, b].astype(F32), bin_ref[1, b].astype(F32)
        level = jnp.full((1, 1), step, jnp.int32).astype(F32) / 64.0
        noisy = (1.0 - level) * noise + level * data
        cond = data * (1.0 - masked)
        inputs = jnp.concatenate([noisy, cond], axis=1).astype(BF16)
        hidden = dot(inputs, win_ref[...])
        hidden_ref[rows] = hidden
        scale = lax.rsqrt(jnp.mean(hidden * hidden, axis=1, keepdims=True) + 1e-06)
        normed = (hidden * scale * gain).astype(BF16)
        normed_ref[rows] = normed
        qkv_ref[rows] = dot(normed, wqkv_ref[...]).astype(BF16)
        return 0

    lax.fori_loop(0, bin_ref.shape[1], block, 0, unroll=2)
    masks = head_masks(width)

    def attend(rows):
        q = qkv_ref[rows, :width] * BF16(HEAD_DIM**-0.5)
        k, v = qkv_ref[rows, width : 2 * width], qkv_ref[rows, 2 * width :]
        out = None
        for m in masks:
            p = softmax(dot(jnp.where(m, q, BF16(0)), k, NT)).astype(BF16)
            o = dot(p, v)
            out = o if out is None else jnp.where(m, o, out)
        att_ref[rows] = out.astype(BF16)

    utterances(utt_ref, longest, attend)


def backward_kernel(
    longest, utt_ref, start_ref, size_ref, bin_ref, hidden_ref, all_ref, out_ref, own_ref, gain_ref,
    vel_ref, qkv_ref, back_ref, d_ref, do_ref,
):
    width = own_ref.shape[0]
    gain = gain_ref[...].astype(F32)

    def block(b, _):
        rows = pl.ds(pl.multiple_of(b * BLOCK, BLOCK), BLOCK)
        masked, _ = span_table(utt_ref, start_ref, size_ref, None, b)
        mixed = None
        for g in range(all_ref.shape[0]):
            part = dot(all_ref[g, rows], out_ref[g * width : (g + 1) * width]).astype(BF16).astype(F32)
            mixed = part if mixed is None else mixed + part
        wide = (hidden_ref[rows] + mixed).astype(BF16).astype(F32)
        rscale = lax.rsqrt(jnp.mean(wide * wide, axis=1, keepdims=True) + 1e-06)
        normalized = wide * rscale
        velocity = dot((normalized * gain).astype(BF16), vel_ref[...])
        target = bin_ref[1, b].astype(F32) - bin_ref[0, b].astype(F32)
        error = (2.0 * masked * (velocity - target)).astype(BF16)
        scaled = dot(error, vel_ref[...], NT) * gain
        back = (
            rscale * (scaled - normalized * jnp.mean(scaled * normalized, axis=1, keepdims=True))
        ).astype(BF16)
        back_ref[rows] = back
        do_ref[rows] = dot(back, own_ref[...], NT).astype(BF16)
        return 0

    lax.fori_loop(0, bin_ref.shape[1], block, 0, unroll=2)
    masks = head_masks(width)
    scale = HEAD_DIM**-0.5

    def pullback(rows):
        q = qkv_ref[rows, :width] * BF16(scale)
        k, v = qkv_ref[rows, width : 2 * width], qkv_ref[rows, 2 * width :]
        do = do_ref[rows]
        dq = dk = dv = None
        for m in masks:
            qh = jnp.where(m, q, BF16(0))
            doh = jnp.where(m, do, BF16(0))
            p = softmax(dot(qh, k, NT))
            dp = dot(doh, v, NT).astype(BF16).astype(F32)
            ds = (p * (dp - jnp.sum(dp * p, axis=1, keepdims=True))).astype(BF16)
            a, b, c = dot(ds, k), dot(ds, qh, TN), dot(p.astype(BF16), doh, TN)
            dq = a if dq is None else jnp.where(m, a, dq)
            dk = b if dk is None else dk + b
            dv = c if dv is None else dv + c
        d_ref[rows, :width] = (dq * scale).astype(BF16)
        d_ref[rows, width : 2 * width] = dk.astype(BF16)
        d_ref[rows, 2 * width :] = dv.astype(BF16)

    utterances(utt_ref, longest, pullback)


def shards(
    dp, mp, noise_blocks, data_blocks, destination, utt_blocks, span_start, span_size, timestep,
    in_weight, norm_gain, qkv_weight, out_proj, final_gain, vel_weight,
):
    per_dev = noise_blocks.shape[0]
    rows = per_dev * BLOCK
    mel = noise_blocks.shape[1] // BLOCK
    lanes = -(-mel // 128) * 128
    features = in_weight.shape[1]
    width = qkv_weight.shape[2]
    longest = min(4, per_dev)
    both = jnp.concatenate([noise_blocks, data_blocks], axis=0).reshape(2, per_dev, BLOCK, mel)
    frames = jnp.pad(both, ((0, 0), (0, 0), (0, 0), (0, lanes - mel)))
    entry = jnp.pad(in_weight.reshape(2, mel, features), ((0, 0), (0, lanes - mel), (0, 0)))
    entry = entry.reshape(2 * lanes, features)
    exit_weight = jnp.pad(vel_weight, ((0, 0), (0, lanes - mel)))
    flat_qkv = qkv_weight.reshape(features, 3 * width)
    dma = pltpu.SemaphoreType.DMA

    def array(shape, kind):
        return jax.ShapeDtypeStruct(shape, kind)

    bins, out_full, count = pl.pallas_call(
        functools.partial(load_kernel, dp, mp),
        out_shape=(
            array(frames.shape, BF16), array((mp * width, features), BF16), array((8, 128), F32),
        ),
        in_specs=[SMEM] * 4 + [VMEM] * 2,
        out_specs=(VMEM,) * 3,
        scratch_shapes=[
            pltpu.VMEM((dp, 2, BLOCK, lanes), BF16),
            pltpu.VMEM((dp, 2, BLOCK, lanes), BF16),
            pltpu.VMEM((dp, 8, 128), F32),
        ] + [dma((dp,))] * 6 + [dma(())] + [dma((mp,))] * 4,
        compiler_params=params(collective_id=0, has_side_effects=True),
        name="load_blocks",
    )(destination, utt_blocks, span_start, span_size, frames, out_proj)
    hidden0, normed, qkv, attended = pl.pallas_call(
        functools.partial(forward_kernel, longest),
        out_shape=(
            array((rows, features), F32), array((rows, features), BF16),
            array((rows, 3 * width), BF16), array((rows, width), BF16),
        ),
        in_specs=[SMEM] * 4 + [VMEM] * 4,
        out_specs=(VMEM,) * 4,
        compiler_params=params(),
        name="forward",
    )(utt_blocks, span_start, span_size, timestep, bins, entry, norm_gain.reshape(1, features), flat_qkv)
    everyone = pl.pallas_call(
        functools.partial(gather_kernel, dp, mp),
        out_shape=array((mp, rows, width), BF16),
        in_specs=[VMEM],
        out_specs=VMEM,
        scratch_shapes=[dma(()), dma((mp,)), dma((mp,)), dma((mp,)), dma((mp,))],
        compiler_params=params(collective_id=1, has_side_effects=True),
        name="gather_attended",
    )(attended)
    back1, grads = pl.pallas_call(
        functools.partial(backward_kernel, longest),
        out_shape=(array((rows, features), BF16), array((rows, 3 * width), BF16)),
        in_specs=[SMEM] * 3 + [VMEM] * 8,
        out_specs=(VMEM,) * 2,
        scratch_shapes=[pltpu.VMEM((rows, width), BF16)],
        compiler_params=params(),
        name="backward",
    )(
        utt_blocks, span_start, span_size, bins, hidden0, everyone, out_full, out_proj,
        final_gain.reshape(1, features), exit_weight, qkv,
    )
    share, groups = features // dp, dp // 2
    summed_qkv, summed_out = pl.pallas_call(
        functools.partial(reduce_kernel, dp, mp),
        out_shape=(array((share, 3 * width), F32), array((share, width), F32)),
        in_specs=[VMEM] * 5,
        out_specs=(VMEM,) * 2,
        scratch_shapes=[
            pltpu.VMEM((4, features, width), BF16),
            pltpu.VMEM((4, groups, share, width), BF16),
            pltpu.VMEM((4, groups, share, width), BF16),
            pltpu.VMEM((4, groups, share, width), BF16),
        ] + [dma((4, groups))] * 4,
        compiler_params=params(collective_id=2, has_side_effects=True),
        name="reduce_grads",
    )(normed, grads, back1, attended, count)
    return (summed_qkv.reshape(share, 3, width), summed_out.T)


def solution(mesh):
    in_specs = (
        P("dp", None), P("dp", None), P(), P("dp", None), P("dp", None), P("dp", None),
        P("dp", None), P(), P(), P(None, None, "mp"), P("mp", None), P(), P(),
    )
    out_specs = (P("dp", None, "mp"), P("mp", "dp"))
    return jax.shard_map(
        functools.partial(shards, mesh.shape["dp"], mesh.shape["mp"]),
        mesh=mesh, in_specs=in_specs, out_specs=out_specs, check_vma=False,
    )
```

```python
import functools

import jax
import jax.numpy as jnp
from jax import lax
from jax.experimental import pallas as pl
from jax.experimental.pallas import tpu as pltpu
from jax.sharding import PartitionSpec as P

HEAD_DIM = 64
BLOCK = 128
MESH = pl.DeviceIdType.MESH
VMEM = pl.BlockSpec(memory_space=pltpu.VMEM)
SMEM = pl.BlockSpec(memory_space=pltpu.SMEM)
F32, BF16 = jnp.float32, jnp.bfloat16
NT = (((1,), (1,)), ((), ()))
TN = (((0,), (0,)), ((), ()))


def dot(a, b, dims=(((1,), (0,)), ((), ()))):
    return lax.dot_general(a, b, dims, preferred_element_type=F32)


def params(**kw):
    return pltpu.CompilerParams(vmem_limit_bytes=56 * 2**20, **kw)


def greet(dp, mp, with_dp, with_mp):
    me, my = lax.axis_index("dp"), lax.axis_index("mp")
    barrier = pltpu.get_barrier_semaphore()
    n = 0
    if with_dp:
        for i in range(1, dp):
            pl.semaphore_signal(
                barrier, inc=1, device_id=(lax.rem(me + i, dp), my), device_id_type=MESH
            )
        n += dp - 1
    if with_mp:
        for i in range(1, mp):
            pl.semaphore_signal(
                barrier, inc=1, device_id=(me, lax.rem(my + i, mp)), device_id_type=MESH
            )
        n += mp - 1
    return lambda: pl.semaphore_wait(barrier, n)


PIECES = 4


def gather_mp(mp, src_at, dst_at, local, send, recv, fsend, frecv):
    me, my = lax.axis_index("dp"), lax.axis_index("mp")
    pair, side = my // 2, lax.rem(my, 2)
    mate = pair * 2 + 1 - side
    direct, keep, near = [], [], []
    for p in range(PIECES):
        keep.append(pltpu.make_async_copy(src_at(p), dst_at(my, p), local.at[p]))
        for c in range(1, mp // 2):
            far = lax.rem(pair + c, mp // 2) * 2 + side
            direct.append((p, c, pltpu.make_async_remote_copy(
                src_at(p), dst_at(my, p), send.at[c, p], recv.at[c, p],
                device_id=(me, far), device_id_type=MESH,
            )))
        near.append(pltpu.make_async_remote_copy(
            src_at(p), dst_at(my, p), send.at[0, p], recv.at[0, p],
            device_id=(me, mate), device_id_type=MESH,
        ))

    def start():
        for _, _, d in direct:
            d.start()
        for n in near + keep:
            n.start()

    def finish():
        onward = []
        for p, c, d in direct:
            d.wait_recv()
            origin = lax.rem(pair + mp // 2 - c, mp // 2) * 2 + side
            f = pltpu.make_async_remote_copy(
                dst_at(origin, p), dst_at(origin, p), fsend.at[c, p], frecv.at[c, p],
                device_id=(me, mate), device_id_type=MESH,
            )
            f.start()
            onward.append(f)
        for n in near + keep:
            n.wait()
        for _, _, d in direct:
            d.wait_send()
        for f in onward:
            f.wait()

    return start, finish


def load_kernel(
    dp, mp, dest_ref, utt_ref, start_ref, size_ref, x_ref, w_ref,
    bin_ref, full_ref, count_ref,
    stage, got, tally, send, recv, csend, crecv, hsend, hrecv, local, ssend, srecv, fsend, frecv,
):
    me, my = lax.axis_index("dp"), lax.axis_index("mp")
    wait = greet(dp, mp, True, True)
    per_dev = bin_ref.shape[1]
    owners = [dest_ref[me * per_dev + k] // per_dev for k in range(per_dev)]
    for i in range(dp):
        to = lax.rem(me + i, dp)
        pick = jnp.int32(0)
        for k in range(per_dev):
            pick = jnp.where(owners[k] == to, k, pick)
        for part in range(2):
            stage[i, part] = x_ref[part, pick]
    count = jnp.int32(0)
    for u in range(utt_ref.shape[1]):
        low = start_ref[0, u]
        high = jnp.minimum(low + size_ref[0, u], 64)
        count += (high - low) * utt_ref[0, u] * (BLOCK // 64)
    tally[me] = jnp.full(tally.shape[1:], count, jnp.int32).astype(F32)
    side = lax.rem(my, 2)
    mate = my + 1 - 2 * side
    half = BLOCK // 2
    lines = pl.ds(pl.multiple_of(side * half, half), half)
    got[me, :, lines] = stage[0, :, lines]
    wait()
    rows = w_ref.shape[0]
    piece = rows // PIECES
    start, finish = gather_mp(
        mp, lambda p: w_ref.at[pl.ds(p * piece, piece)],
        lambda i, p: full_ref.at[pl.ds(pl.multiple_of(i * rows + p * piece, piece), piece)],
        local, ssend, srecv, fsend, frecv,
    )
    frames, counts = [], []
    for i in range(1, dp):
        to = lax.rem(me + i, dp)
        frames.append(
            pltpu.make_async_remote_copy(
                stage.at[i, :, lines], got.at[me, :, lines], send.at[i], recv.at[i],
                device_id=(to, my), device_id_type=MESH,
            )
        )
        counts.append(
            pltpu.make_async_remote_copy(
                tally.at[me], tally.at[me], csend.at[i], crecv.at[i],
                device_id=(to, my), device_id_type=MESH,
            )
        )
    for c in frames + counts:
        c.start()
    start()
    onward = []
    for i in range(dp):
        if i > 0:
            frames[i - 1].wait_recv()
        slot = lax.rem(me + dp - i, dp)
        f = pltpu.make_async_remote_copy(
            got.at[slot, :, lines], got.at[slot, :, lines], hsend.at[i], hrecv.at[i],
            device_id=(me, mate), device_id_type=MESH,
        )
        f.start()
        onward.append(f)

    def find(i, found):
        d = dest_ref[i]
        return tuple(jnp.where(d == me * per_dev + j, i // per_dev, o) for j, o in enumerate(found))

    origin = lax.fori_loop(0, dp * per_dev, find, (jnp.int32(0),) * per_dev)
    finish()
    for c in frames:
        c.wait_send()
    for c in counts + onward:
        c.wait()
    for j in range(per_dev):
        for part in range(2):
            bin_ref[part, j] = got[origin[j], part]
    count_ref[...] = jnp.sum(tally[...], axis=0)


def gather_kernel(dp, mp, a_ref, out_ref, local, send, recv, fsend, frecv):
    greet(dp, mp, False, True)()
    piece = a_ref.shape[0] // PIECES
    start, finish = gather_mp(
        mp, lambda p: a_ref.at[pl.ds(p * piece, piece)],
        lambda i, p: out_ref.at[i, pl.ds(p * piece, piece)], local, send, recv, fsend, frecv,
    )
    start()
    finish()


def reduce_kernel(
    dp, mp, normed_ref, d_ref, back_ref, att_ref, count_ref, qkv_out, o_out,
    terms, near, sums, far, s1, r1, s2, r2,
):
    me, my = lax.axis_index("dp"), lax.axis_index("mp")
    ready = greet(dp, mp, True, False)
    rows, chunks, groups = o_out.shape[0], terms.shape[0], dp // 2
    group, side = me // 2, lax.rem(me, 2)
    mate = me + 1 - 2 * side
    width = o_out.shape[1]

    def block(j, g, s):
        return terms.at[j, pl.ds(pl.multiple_of((g * 2 + s) * rows, rows), rows)]

    first, second = [], []

    def middle(j):
        for i in range(1, groups):
            g = lax.rem(group + i, groups)
            first[j][i].wait_recv()
            sums[j, i] = (block(j, g, side)[...].astype(F32) + near[j, g].astype(F32)).astype(BF16)
            c = pltpu.make_async_remote_copy(
                sums.at[j, i], far.at[j, i], s2.at[j, i], r2.at[j, i],
                device_id=(g * 2 + side, my), device_id_type=MESH,
            )
            c.start()
            second.append(c)
        first[j][0].wait_recv()

    def last(j):
        total = block(j, group, side)[...].astype(F32) + near[j, group].astype(F32)
        for i in range(1, groups):
            second[j * (groups - 1) + i - 1].wait_recv()
            total += far[j, i].astype(F32)
        total = total / count_ref[0:1, :]
        if j == 0:
            o_out[...] = total.T if o_out.shape[0] == width else total
        else:
            qkv_out[j - 1] = total

    for j in range(chunks):
        if j == 0:
            t = dot(att_ref[...], back_ref[...], TN).T
        else:
            t = dot(d_ref[:, (j - 1) * width : j * width], normed_ref[...], TN).T
        terms[j] = t.astype(BF16)
        if j == 0:
            ready()
        out = []
        for i in range(groups):
            g = lax.rem(group + i, groups)
            out.append(
                pltpu.make_async_remote_copy(
                    block(j, g, 1 - side), near.at[j, g], s1.at[j, i], r1.at[j, i],
                    device_id=(mate, my), device_id_type=MESH,
                )
            )
        for c in out[1:] + out[:1]:
            c.start()
        first.append(out)
        if j > 0:
            middle(j - 1)
    middle(chunks - 1)
    for j in range(chunks):
        last(j)
    for out in first:
        for c in out:
            c.wait_send()
    for c in second:
        c.wait_send()


def utterances(utt_ref, longest, body):
    def step(u, at):
        length = utt_ref[0, u]
        for n in range(1, longest + 1):
            @pl.when(length == n)
            def _():
                body(pl.ds(pl.multiple_of(at * BLOCK, BLOCK), n * BLOCK))
        return at + length

    lax.fori_loop(0, utt_ref.shape[1], step, jnp.int32(0))


def span_table(utt_ref, start_ref, size_ref, step_ref, b):
    at = jnp.int32(0)
    offset = low = high = step = jnp.int32(0)
    for u in range(utt_ref.shape[1]):
        n = utt_ref[0, u]
        inside = (b >= at) & (b < at + n)
        lo = start_ref[0, u] * n * (BLOCK // 64)
        hi = (start_ref[0, u] + size_ref[0, u]) * n * (BLOCK // 64)
        offset = jnp.where(inside, (b - at) * BLOCK, offset)
        low = jnp.where(inside, lo, low)
        high = jnp.where(inside, hi, high)
        if step_ref is not None:
            step = jnp.where(inside, step_ref[0, u], step)
        at = at + n
    frame = offset + lax.broadcasted_iota(jnp.int32, (BLOCK, 1), 0)
    masked = ((frame >= low) & (frame < high)).astype(F32)
    return masked, step


def head_masks(width):
    lane = lax.broadcasted_iota(jnp.int32, (1, width), 1) // HEAD_DIM
    return [lane == h for h in range(width // HEAD_DIM)]


def softmax(s):
    e = jnp.exp(s - jnp.max(s, axis=1, keepdims=True))
    return e / jnp.sum(e, axis=1, keepdims=True)


def forward_kernel(
    longest, utt_ref, start_ref, size_ref, step_ref, bin_ref, win_ref, gain_ref, wqkv_ref,
    hidden_ref, normed_ref, qkv_ref, att_ref,
):
    width = att_ref.shape[1]
    gain = gain_ref[...].astype(F32).reshape(1, -1)

    def block(b, _):
        rows = pl.ds(pl.multiple_of(b * BLOCK, BLOCK), BLOCK)
        masked, step = span_table(utt_ref, start_ref, size_ref, step_ref, b)
        noise, data = bin_ref[0, b].astype(F32), bin_ref[1, b].astype(F32)
        level = jnp.full((1, 1), step, jnp.int32).astype(F32) / 64.0
        noisy = (1.0 - level) * noise + level * data
        cond = data * (1.0 - masked)
        inputs = jnp.concatenate([noisy, cond], axis=1).astype(BF16)
        hidden = dot(inputs, win_ref[...])
        hidden_ref[rows] = hidden
        scale = lax.rsqrt(jnp.mean(hidden * hidden, axis=1, keepdims=True) + 1e-06)
        normed = (hidden * scale * gain).astype(BF16)
        normed_ref[rows] = normed
        for j in range(3):
            qkv_ref[rows, j * width : (j + 1) * width] = dot(normed, wqkv_ref[j]).astype(BF16)
        return 0

    lax.fori_loop(0, bin_ref.shape[1], block, 0, unroll=2)
    masks = head_masks(width)

    def attend(rows):
        q = qkv_ref[rows, :width] * BF16(HEAD_DIM**-0.5)
        k, v = qkv_ref[rows, width : 2 * width], qkv_ref[rows, 2 * width :]
        out = None
        for m in masks:
            p = softmax(dot(jnp.where(m, q, BF16(0)), k, NT)).astype(BF16)
            o = dot(p, v)
            out = o if out is None else jnp.where(m, o, out)
        att_ref[rows] = out.astype(BF16)

    utterances(utt_ref, longest, attend)


def backward_kernel(
    longest, utt_ref, start_ref, size_ref, bin_ref, hidden_ref, all_ref, out_ref, own_ref, gain_ref,
    vel_ref, qkv_ref, back_ref, d_ref, do_ref,
):
    width = own_ref.shape[0]
    gain = gain_ref[...].astype(F32).reshape(1, -1)

    def block(b, _):
        rows = pl.ds(pl.multiple_of(b * BLOCK, BLOCK), BLOCK)
        masked, _ = span_table(utt_ref, start_ref, size_ref, None, b)
        mixed = None
        for g in range(all_ref.shape[0]):
            part = dot(all_ref[g, rows], out_ref[g * width : (g + 1) * width]).astype(BF16).astype(F32)
            mixed = part if mixed is None else mixed + part
        wide = (hidden_ref[rows] + mixed).astype(BF16).astype(F32)
        rscale = lax.rsqrt(jnp.mean(wide * wide, axis=1, keepdims=True) + 1e-06)
        normalized = wide * rscale
        velocity = dot((normalized * gain).astype(BF16), vel_ref[...], NT)
        target = bin_ref[1, b].astype(F32) - bin_ref[0, b].astype(F32)
        error = (2.0 * masked * (velocity - target)).astype(BF16)
        scaled = dot(error, vel_ref[...]) * gain
        back = (
            rscale * (scaled - normalized * jnp.mean(scaled * normalized, axis=1, keepdims=True))
        ).astype(BF16)
        back_ref[rows] = back
        do_ref[rows] = dot(back, own_ref[...], NT).astype(BF16)
        return 0

    lax.fori_loop(0, bin_ref.shape[1], block, 0, unroll=2)
    masks = head_masks(width)
    scale = HEAD_DIM**-0.5

    def pullback(rows):
        q = qkv_ref[rows, :width] * BF16(scale)
        k, v = qkv_ref[rows, width : 2 * width], qkv_ref[rows, 2 * width :]
        do = do_ref[rows]
        dq = dk = dv = None
        for m in masks:
            qh = jnp.where(m, q, BF16(0))
            doh = jnp.where(m, do, BF16(0))
            p = softmax(dot(qh, k, NT))
            dp = dot(doh, v, NT).astype(BF16).astype(F32)
            ds = (p * (dp - jnp.sum(dp * p, axis=1, keepdims=True))).astype(BF16)
            a, b, c = dot(ds, k), dot(ds, qh, TN), dot(p.astype(BF16), doh, TN)
            dq = a if dq is None else jnp.where(m, a, dq)
            dk = b if dk is None else dk + b
            dv = c if dv is None else dv + c
        d_ref[rows, :width] = (dq * scale).astype(BF16)
        d_ref[rows, width : 2 * width] = dk.astype(BF16)
        d_ref[rows, 2 * width :] = dv.astype(BF16)

    utterances(utt_ref, longest, pullback)


def shards(
    dp, mp, noise_blocks, data_blocks, destination, utt_blocks, span_start, span_size, timestep,
    in_weight, norm_gain, qkv_weight, out_proj, final_gain, vel_weight,
):
    per_dev = noise_blocks.shape[0]
    rows = per_dev * BLOCK
    mel = noise_blocks.shape[1] // BLOCK
    features = in_weight.shape[1]
    width = qkv_weight.shape[2]
    longest = min(4, per_dev)
    frames = jnp.concatenate([noise_blocks, data_blocks], axis=0).reshape(2, per_dev, BLOCK, mel)
    dma = pltpu.SemaphoreType.DMA

    def array(shape, kind):
        return jax.ShapeDtypeStruct(shape, kind)

    bins, out_full, count = pl.pallas_call(
        functools.partial(load_kernel, dp, mp),
        out_shape=(
            array(frames.shape, BF16), array((mp * width, features), BF16), array((8, 128), F32),
        ),
        in_specs=[SMEM] * 4 + [VMEM] * 2,
        out_specs=(VMEM,) * 3,
        scratch_shapes=[
            pltpu.VMEM((dp, 2, BLOCK, mel), BF16),
            pltpu.VMEM((dp, 2, BLOCK, mel), BF16),
            pltpu.VMEM((dp, 8, 128), F32),
        ] + [dma((dp,))] * 6 + [dma((PIECES,))] + [dma((mp, PIECES))] * 4,
        compiler_params=params(collective_id=0, has_side_effects=True),
        name="load_blocks",
    )(destination, utt_blocks, span_start, span_size, frames, out_proj)
    hidden0, normed, qkv, attended = pl.pallas_call(
        functools.partial(forward_kernel, longest),
        out_shape=(
            array((rows, features), F32), array((rows, features), BF16),
            array((rows, 3 * width), BF16), array((rows, width), BF16),
        ),
        in_specs=[SMEM] * 4 + [VMEM] * 4,
        out_specs=(VMEM,) * 4,
        compiler_params=params(),
        name="forward",
    )(utt_blocks, span_start, span_size, timestep, bins, in_weight, norm_gain, qkv_weight.transpose(1, 0, 2))
    everyone = pl.pallas_call(
        functools.partial(gather_kernel, dp, mp),
        out_shape=array((mp, rows, width), BF16),
        in_specs=[VMEM],
        out_specs=VMEM,
        scratch_shapes=[dma((PIECES,))] + [dma((mp, PIECES))] * 4,
        compiler_params=params(collective_id=1, has_side_effects=True),
        name="gather_attended",
    )(attended)
    back1, grads = pl.pallas_call(
        functools.partial(backward_kernel, longest),
        out_shape=(array((rows, features), BF16), array((rows, 3 * width), BF16)),
        in_specs=[SMEM] * 3 + [VMEM] * 8,
        out_specs=(VMEM,) * 2,
        scratch_shapes=[pltpu.VMEM((rows, width), BF16)],
        compiler_params=params(),
        name="backward",
    )(
        utt_blocks, span_start, span_size, bins, hidden0, everyone, out_full, out_proj,
        final_gain, vel_weight.T, qkv,
    )
    share, groups = features // dp, dp // 2
    summed_qkv, summed_out = pl.pallas_call(
        functools.partial(reduce_kernel, dp, mp),
        out_shape=(array((3, share, width), F32), array((share, width), F32)),
        in_specs=[VMEM] * 5,
        out_specs=(VMEM,) * 2,
        scratch_shapes=[
            pltpu.VMEM((4, features, width), BF16),
            pltpu.VMEM((4, groups, share, width), BF16),
            pltpu.VMEM((4, groups, share, width), BF16),
            pltpu.VMEM((4, groups, share, width), BF16),
        ] + [dma((4, groups))] * 4,
        compiler_params=params(collective_id=2, has_side_effects=True),
        name="reduce_grads",
    )(normed, grads, back1, attended, count)
    return (
        summed_qkv.transpose(1, 0, 2),
        summed_out if share == width else summed_out.T,
    )


def solution(mesh):
    in_specs = (
        P("dp", None), P("dp", None), P(), P("dp", None), P("dp", None), P("dp", None),
        P("dp", None), P(), P(), P(None, None, "mp"), P("mp", None), P(), P(),
    )
    out_specs = (P("dp", None, "mp"), P("mp", "dp"))
    return jax.shard_map(
        functools.partial(shards, mesh.shape["dp"], mesh.shape["mp"]),
        mesh=mesh, in_specs=in_specs, out_specs=out_specs, check_vma=False,
    )
```
